32 devices in a mesh: dp: 1, cp: 32 (over z, y, x, core).
Axes of the slice: x: 2, y: 2, z: 4, core: 2. Of those that a mesh axis runs over, the one named last changes fastest.
Arguments:
- hidden: bfloat16 [1, 4096, 2880], P('dp', 'cp'), may hold values from -8 to 8
- norm_gain: float32 [2880], replicated, may hold values from 0.5 to 1.5
- query_weight: bfloat16 [2880, 2048], replicated, may hold values from -4 to 4
- keyval_weight: bfloat16 [2880, 512], replicated, may hold values from -1 to 1
- sink_logits: float32 [32], replicated, may hold values from -1 to 3
- document_ids: int32 [1, 4096], P('dp', 'cp'), may hold values from 0 to 15, never falling along the last dimension, each value on 1 to 1024 neighbouring positions
- block_owner: int32 [1, 32, 32], P('dp', 'cp'), may hold values from 0 to 31, each once within a row
- loss_mask: int32 [1, 4096], P('dp', 'cp'), may hold values from 0 to 1, as said below
Outputs:
- attended: bfloat16 [1, 4096, 2048], P('dp', 'cp')
- row_lse: float32 [1, 32, 4096], P('dp', None, 'cp')
- token_weight: float32 [1, 4096], P('dp', 'cp')
The draws below stay inside these ranges and needn't reach their ends.
Inputs may be any that keep to these rules, and one draw needn't show every extreme that they name: `document_ids`: in each group the ids start at 0, never fall, rise by at most one from a position to the next and end at 15; a document holds at most 1024 positions. `block_owner`: for each group and device the row of 32 entries is a permutation of 0 to 31. `loss_mask`: the last flag of each group is 1.
All inputs are finite; a program needn't handle non-finite values.
Results may differ from the reference program's by a relative error of at most 0.008.
Values may be sent and summed in bfloat16 or wider, within the bound.
A program may use at most 128 MiB of HBM per device.

```python
import math
import jax
import jax.numpy as jnp
import numpy as np
from jax import lax

D = 2880
HEAD_DIM = 64
HEADS = 32
KV_HEADS = 4
TOK_DEV = 128
QDIM = 2048
KVDIM = 256
SHARDS = 32
GROUPS = 1
GTOK = 4096
BLOCK = 4
DOCS = 16
DOC_MOST = 1024


def shared_keyval(key):
    base_draw = jax.random.normal(jax.random.fold_in(key, 5), (D, 2 * KVDIM), jnp.float32) * D ** (-0.5)
    return jnp.clip(base_draw, -1.0, 1.0)


def draw_keyval_weight(key, part):
    return shared_keyval(key).astype(jnp.bfloat16)


def draw_query_weight(key, part):
    base_draw = jax.random.normal(jax.random.fold_in(key, 7), (D, QDIM), jnp.float32) * D ** (-0.5)
    return jnp.clip(base_draw, -4.0, 4.0).astype(jnp.bfloat16)


def draw_hidden(key, part):
    base_draw = jax.random.normal(jax.random.fold_in(key, 3), (GROUPS, GTOK, D), jnp.float32)
    return jnp.clip(base_draw, -8.0, 8.0).astype(jnp.bfloat16)


def draw_loss_mask(key, part):
    places = jnp.arange(GROUPS * GTOK, dtype=jnp.int32).reshape(GROUPS, GTOK)
    threshold = 200 + 600 * places // (GROUPS * GTOK)
    drawn = jax.random.randint(jax.random.fold_in(key, 9), (GROUPS, GTOK), 0, 1000, dtype=jnp.int32)
    flag_values = (drawn < threshold).astype(jnp.int32)
    return flag_values.at[:, -1].set(1)


def profile(amount, total, most, lean):
    loads = [(1 << 20) // math.isqrt(rank ** lean) + 1 for rank in range(2, amount + 1)]
    rest, holding = total - most - (amount - 1), [1] * (amount - 1)
    while rest > 0:
        movable = [i for i in range(amount - 1) if holding[i] < most]
        whole, remaining = sum([loads[i] for i in movable]), rest
        for i in movable:
            extra = min(most - holding[i], max(1, remaining * loads[i] // whole), rest)
            holding[i] = holding[i] + extra
            rest = rest - extra
    return np.array([most] + holding)


def uneven(own_key, number_of, total, limit, skew):
    if number_of == 2:
        one = jax.random.randint(own_key, (), max(1, total - limit), min(limit, total - 1) + 1)
        return jnp.stack([one, total - one])
    lengths = jnp.asarray(profile(number_of, total, limit, skew), jnp.int32)
    twos = (number_of - 1) // 2
    giver, taker = lengths[1:1 + 2 * twos:2], lengths[2:2 + 2 * twos:2]
    slack = jnp.minimum(giver - 1, limit - taker)
    shifted = jax.random.randint(jax.random.fold_in(own_key, 1), (twos,), 0, 1 << 20) % (slack + 1)
    lengths = lengths.at[1:1 + 2 * twos:2].set(giver - shifted).at[2:2 + 2 * twos:2].set(taker + shifted)
    return lengths[jax.random.permutation(jax.random.fold_in(own_key, 2), number_of)]


def setup_inputs(seed: int = 0) -> dict:
    seeds = jax.random.split(jax.random.key(seed), 9)
    return {
        "hidden": draw_hidden(jax.random.fold_in(seeds[8], 71), 0),
        "norm_gain": jnp.clip(1.0 + 0.1 * jax.random.normal(seeds[1], (D,), jnp.float32), 0.5, 1.5),
        "query_weight": draw_query_weight(jax.random.fold_in(seeds[8], 71), 0),
        "keyval_weight": draw_keyval_weight(jax.random.fold_in(seeds[8], 71), 0),
        "sink_logits": jnp.clip(jax.random.uniform(seeds[4], (HEADS,), jnp.float32, -1.0, 3.0), -1.0, 3.0),
        "document_ids": jax.vmap(lambda own: jnp.searchsorted(jnp.cumsum(uneven(own, DOCS, GTOK, DOC_MOST, 2)), jnp.arange(GTOK), side="right"))(jax.random.split(seeds[5], GROUPS)).reshape((GROUPS, GTOK)).astype(jnp.int32),
        "block_owner": jax.vmap(lambda own: jax.random.permutation(own, SHARDS))(jax.random.split(seeds[6], GROUPS * SHARDS)).reshape((GROUPS, SHARDS, SHARDS)).astype(jnp.int32),
        "loss_mask": draw_loss_mask(jax.random.fold_in(seeds[8], 71), 0),
    }


rope_base = 150000.0
norm_eps = 1e-05
masked_score = -1e+30

def rotate(values, within):
    half_dim = values.shape[-1] // 2
    frequency = jnp.power(rope_base, -jnp.arange(half_dim, dtype=jnp.float32) / half_dim)
    angles = within.astype(jnp.float32)[:, None, None] * frequency[None, None, :]
    cosine = jnp.cos(angles)
    sine_part = jnp.sin(angles)
    first = values[..., :half_dim]
    second = values[..., half_dim:]
    return jnp.concatenate([first * cosine - second * sine_part, second * cosine + first * sine_part], axis=-1)

def doc_within(doc_index):
    length = doc_index.shape[0]
    places = jnp.arange(length, dtype=jnp.int32)
    fresh_doc = jnp.concatenate([jnp.ones((1,), dtype=bool), doc_index[1:] != doc_index[:-1]])
    starts = lax.cummax(jnp.where(fresh_doc, places, 0), axis=0)
    return (places - starts).astype(jnp.int32)

def one_group(rows, doc_index, owner_rows, norm_gain, query_weight, keyval_weight, sink_logits):
    rows_float = rows.astype(jnp.float32)
    inv_rms = lax.rsqrt(lax.optimization_barrier(jnp.mean(rows_float * rows_float, axis=1, keepdims=True)) + norm_eps)
    normed = (rows_float * inv_rms * norm_gain).astype(jnp.bfloat16)
    within = doc_within(doc_index)
    projected = jnp.dot(normed, query_weight, preferred_element_type=jnp.float32).reshape(GTOK, HEADS, HEAD_DIM)
    queries = rotate(projected, within).astype(jnp.bfloat16)
    keyval = jnp.dot(normed, keyval_weight, preferred_element_type=jnp.float32)
    keys_rot = rotate(keyval[:, :KVDIM].reshape(GTOK, KV_HEADS, HEAD_DIM), within).astype(jnp.bfloat16)
    values = keyval[:, KVDIM:].reshape(GTOK, KV_HEADS, HEAD_DIM).astype(jnp.bfloat16)
    group_size = HEADS // KV_HEADS
    keys_float = keys_rot.astype(jnp.float32)
    values_float = values.astype(jnp.float32)
    places = jnp.arange(GTOK, dtype=jnp.int32)
    query_rows = min(512, GTOK)
    score_scale = HEAD_DIM ** (-0.5)

    def query_block(first_row):
        query_part = lax.dynamic_slice_in_dim(queries, first_row, query_rows, 0).astype(jnp.float32)
        query_part = query_part.reshape(query_rows, KV_HEADS, group_size, HEAD_DIM)
        scores = jnp.einsum('qagd,kad->agqk', query_part, keys_float).reshape(HEADS, query_rows, GTOK) * score_scale
        query_place = first_row + jnp.arange(query_rows, dtype=jnp.int32)
        query_doc = lax.dynamic_slice_in_dim(doc_index, first_row, query_rows, 0)
        allowed = (query_doc[:, None] == doc_index[None, :]) & (places[None, :] <= query_place[:, None])
        scores = jnp.where(allowed[None], scores, masked_score)
        row_top = jnp.maximum(sink_logits[:, None], lax.optimization_barrier(jnp.max(scores, axis=-1)))
        exp_scores = jnp.exp(scores - row_top[..., None])
        row_total = jnp.exp(sink_logits[:, None] - row_top) + lax.optimization_barrier(jnp.sum(exp_scores, axis=-1))
        rounded = lax.optimization_barrier(exp_scores.astype(jnp.bfloat16))
        weights = rounded.astype(jnp.float32).reshape(KV_HEADS, group_size, query_rows, GTOK)
        mixed_values = jnp.einsum('agqk,kad->agqd', weights, values_float).reshape(HEADS, query_rows, HEAD_DIM)
        normalized = mixed_values / row_total[..., None]
        normalized = jnp.transpose(normalized, (1, 0, 2)).reshape(query_rows, QDIM).astype(jnp.bfloat16)
        return (normalized, row_top + jnp.log(row_total))
    starts = jnp.arange(0, GTOK, query_rows, dtype=jnp.int32)
    outputs, log_totals = lax.map(query_block, starts)
    attended = outputs.reshape(GTOK, QDIM)
    log_total = jnp.transpose(log_totals, (1, 0, 2)).reshape(HEADS, GTOK)
    inverse = jnp.argsort(owner_rows, axis=1).astype(jnp.int32)
    source_shard = jnp.arange(SHARDS, dtype=jnp.int32)[None, :, None]
    inner_rows = jnp.arange(BLOCK, dtype=jnp.int32)[None, None, :]
    source = source_shard * TOK_DEV + jnp.transpose(inverse)[:, :, None] * BLOCK + inner_rows
    row_lse = jnp.take(log_total, source.reshape(-1).astype(jnp.int32), axis=1)
    return (attended, row_lse)

def reference(hidden, norm_gain, query_weight, keyval_weight, sink_logits, document_ids, block_owner, loss_mask):
    attended_list = []
    lse_list = []
    for group_index in range(GROUPS):
        attended, row_lse = one_group(hidden[group_index], document_ids[group_index], block_owner[group_index], norm_gain, query_weight, keyval_weight, sink_logits)
        attended_list.append(attended)
        lse_list.append(row_lse)
    flag_values = loss_mask.astype(jnp.float32)
    token_total = jnp.sum(flag_values)
    token_weight = flag_values * (float(GROUPS * GTOK) / token_total)
    return (jnp.stack(attended_list), jnp.stack(lse_list), token_weight)
```

```python
import functools
import math

import jax
import jax.numpy as jnp
import numpy as np
from jax import lax
from jax.experimental import pallas as pl
from jax.experimental.pallas import tpu as pltpu
from jax.sharding import PartitionSpec as P

HEAD_DIM = 64
DOC_MOST = 1024

rope_base = 150000.0
norm_eps = 1e-05
masked_score = -1e30
LANES = 128
LOG2E = math.log2(math.e)
LN2 = math.log(2.0)
MESH = pl.DeviceIdType.MESH
EXACT = lax.Precision.HIGHEST


def iota(shape, axis):
    return lax.broadcasted_iota(jnp.int32, shape, axis)


def rope_tables(shards, own_rows):
    half = HEAD_DIM // 2
    frequency = rope_base ** (-np.arange(half, dtype=np.float64) / half)
    frequency = np.tile(frequency, LANES // half)
    base = np.arange(shards, dtype=np.float64)[:, None] * own_rows * frequency
    row = np.arange(own_rows, dtype=np.float64)[:, None] * frequency
    return [np.asarray(f(x), np.float32) for x in (base, row) for f in (np.cos, np.sin)]


def kernel(
    dims,
    hidden,
    gain,
    wq_hbm,
    wkv_hbm,
    sink,
    ids,
    owner,
    flags,
    cos_base,
    sin_base,
    cos_row,
    sin_row,
    attended,
    row_lse,
    token_weight,
    wq,
    wkv,
    kv,
    idbuf,
    mkbuf,
    queries,
    bias,
    lse,
    lse_out,
    lse_in,
    w_sem,
    kv_send,
    kv_recv,
    id_send,
    id_recv,
    mk_send,
    mk_recv,
    lse_send,
    lse_recv,
):
    parts, shards, reach, heads, kv_heads = dims
    me = lax.axis_index("cp")
    part = lax.axis_index("dp")
    total = parts * shards
    place = part * shards + me
    rows = hidden.shape[1]
    group = heads // kv_heads
    width = group * HEAD_DIM
    kv_width = kv_heads * HEAD_DIM
    pairs = heads // 2
    pairs_kv = group // 2
    block_rows = rows // shards
    row_bits = block_rows.bit_length() - 1
    head_bits = heads.bit_length() - 1

    def other(off):
        target = lax.rem(place + off, total)
        return {"dp": target // shards, "cp": lax.rem(target, shards)}

    barrier = pltpu.get_barrier_semaphore()

    @pl.loop(1, total)
    def _(off):
        pl.semaphore_signal(barrier, inc=1, device_id=other(off), device_id_type=MESH)

    kv_load = pltpu.make_async_copy(wkv_hbm, wkv, w_sem.at[kv_heads])
    kv_load.start()
    q_loads = [
        pltpu.make_async_copy(wq_hbm.at[:, pl.ds(c * width, width)], wq.at[c], w_sem.at[c])
        for c in range(kv_heads)
    ]
    for load in q_loads:
        load.start()

    def kv_copy(k, target):
        return pltpu.make_async_remote_copy(
            src_ref=kv.at[reach],
            dst_ref=kv.at[reach - k],
            send_sem=kv_send.at[k - 1],
            recv_sem=kv_recv.at[k - 1],
            device_id={"cp": target},
            device_id_type=MESH,
        )

    def id_copy(k, target):
        return pltpu.make_async_remote_copy(
            src_ref=ids,
            dst_ref=idbuf.at[reach - k],
            send_sem=id_send.at[k - 1],
            recv_sem=id_recv.at[k - 1],
            device_id={"cp": target},
            device_id_type=MESH,
        )

    def mk_copy(off):
        return pltpu.make_async_remote_copy(
            src_ref=flags,
            dst_ref=mkbuf.at[off],
            send_sem=mk_send.at[off - 1],
            recv_sem=mk_recv.at[off - 1],
            device_id=other(off),
            device_id_type=MESH,
        )

    def lse_copy(off):
        target = lax.rem(me + off, shards)
        return pltpu.make_async_remote_copy(
            src_ref=lse_out.at[target],
            dst_ref=lse_in.at[me],
            send_sem=lse_send.at[off - 1],
            recv_sem=lse_recv.at[off - 1],
            device_id={"cp": target},
            device_id_type=MESH,
        )

    x = hidden[0].astype(jnp.float32)
    inv_rms = lax.rsqrt(jnp.mean(x * x, axis=1, keepdims=True) + norm_eps)
    normed = (x * inv_rms * gain[...]).astype(jnp.bfloat16)

    cb, sb = cos_base[pl.ds(me, 1), :], sin_base[pl.ds(me, 1), :]
    cr, sr = cos_row[...], sin_row[...]
    lane = iota((rows, LANES), 1)
    first_half = (lane & (HEAD_DIM - 1)) < HEAD_DIM // 2
    low = lane < HEAD_DIM
    cosine = cb * cr - sb * sr
    sine = sb * cr + cb * sr
    sine = jnp.where(first_half, -sine, sine)

    def rotate(u):
        swapped = jnp.where(
            first_half,
            pltpu.roll(u, LANES - HEAD_DIM // 2, 1),
            pltpu.roll(u, HEAD_DIM // 2, 1),
        )
        return u * cosine + swapped * sine

    kv_load.wait()
    keyval = jnp.dot(normed, wkv[...], preferred_element_type=jnp.float32)
    for c in range(kv_width // LANES):
        part_k = keyval[:, c * LANES : (c + 1) * LANES]
        kv[reach, c * LANES : (c + 1) * LANES, :] = rotate(part_k).astype(jnp.bfloat16)
        part_v = keyval[:, kv_width + c * LANES : kv_width + (c + 1) * LANES]
        kv[reach, kv_width + c * LANES : kv_width + (c + 1) * LANES, :] = part_v.T.astype(
            jnp.bfloat16
        )
    idbuf[reach] = ids[...]
    mkbuf[0] = flags[...]

    pl.semaphore_wait(barrier, total - 1)

    @pl.loop(1, reach + 1)
    def _(k):
        @pl.when(me + k < shards)
        def _():
            id_copy(k, me + k).start()
            kv_copy(k, me + k).start()

        @pl.when(me - k < 0)
        def _():
            kv[reach - k] = jnp.zeros(kv.shape[1:], kv.dtype)
            idbuf[reach - k] = jnp.full(idbuf.shape[1:], -1, jnp.int32)

    @pl.loop(1, total)
    def _(off):
        mk_copy(off).start()

    for c in range(kv_heads):
        q_loads[c].wait()
        projected = jnp.dot(normed, wq[c], preferred_element_type=jnp.float32)
        for j in range(pairs_kv):
            y = rotate(projected[:, j * LANES : (j + 1) * LANES]) * (LOG2E * HEAD_DIM**-0.5)
            yr = pltpu.roll(y, HEAD_DIM, 1)
            if c % 2 == 0:
                one, two = jnp.where(low, y, 0.0), jnp.where(low, yr, 0.0)
            else:
                one, two = jnp.where(low, 0.0, yr), jnp.where(low, 0.0, y)
            queries[c * pairs_kv + j, 0:rows, :] = one.astype(jnp.bfloat16)
            queries[c * pairs_kv + j, rows : 2 * rows, :] = two.astype(jnp.bfloat16)

    @pl.loop(1, reach + 1)
    def _(k):
        @pl.when(me - k >= 0)
        def _():
            id_copy(k, me).wait_recv()

    own_ids = jnp.broadcast_to(ids[...].astype(jnp.float32), (rows, rows))
    for slot in range(reach + 1):
        key_ids = jnp.broadcast_to(idbuf[slot].astype(jnp.float32), (rows, rows)).T
        allowed = key_ids == own_ids
        if slot == reach:
            allowed = allowed & (iota((rows, rows), 0) <= iota((rows, rows), 1))
        bias[slot * rows : (slot + 1) * rows, :] = jnp.where(allowed, 0.0, masked_score)

    @pl.loop(1, reach + 1)
    def _(k):
        @pl.when(me - k >= 0)
        def _():
            kv_copy(k, me).wait_recv()

    key_count = (reach + 1) * rows

    def attend(p):
        a = p // pairs_kv
        key_part = kv[:, pl.ds(pl.multiple_of((a // 2) * LANES, LANES), LANES), :]
        key_part = key_part.reshape(key_count, LANES)
        value_rows = pl.ds(pl.multiple_of(kv_width + a * HEAD_DIM, HEAD_DIM), HEAD_DIM)
        values_t = jnp.concatenate([kv[s, value_rows, :] for s in range(reach + 1)], axis=1)
        scores = lax.dot_general(
            key_part, queries[p], (((1,), (1,)), ((), ())), preferred_element_type=jnp.float32
        )
        shift = bias[...]
        scores = scores + jnp.concatenate([shift, shift], axis=1)
        sink_row = jnp.where(
            iota((1, 2 * rows), 1) < rows, sink[2 * p] * LOG2E, sink[2 * p + 1] * LOG2E
        )
        top = jnp.maximum(jnp.max(scores, axis=0, keepdims=True), sink_row)
        weights = jnp.exp2(scores - top)
        row_total = jnp.sum(weights, axis=0, keepdims=True) + jnp.exp2(sink_row - top)
        mixed = jnp.dot(
            values_t, weights.astype(jnp.bfloat16), preferred_element_type=jnp.float32
        )
        mixed = mixed / row_total
        both = jnp.concatenate([mixed[:, :rows], mixed[:, rows:]], axis=0)
        attended[0, :, pl.ds(pl.multiple_of(p * LANES, LANES), LANES)] = both.T.astype(
            jnp.bfloat16
        )
        log_total = top * LN2 + jnp.log(row_total)
        lse[pl.ds(2 * p, 1), :] = log_total[:, :rows]
        lse[pl.ds(2 * p + 1, 1), :] = log_total[:, rows:]

    @pl.loop(0, pairs // 2)
    def _(i):
        attend(2 * i)
        attend(2 * i + 1)

    wide = block_rows * heads
    owner_hot = (jnp.broadcast_to(owner[0], (shards, shards)) == iota((shards, shards), 0)).astype(
        jnp.float32
    )
    spread = ((iota((shards, rows), 1) >> row_bits) == iota((shards, rows), 0)).astype(jnp.float32)
    takes = jnp.dot(owner_hot, spread, preferred_element_type=jnp.float32)
    inner = iota((heads, rows), 1) & (block_rows - 1)
    lse_all = lse[...]
    stacked = jnp.concatenate(
        [jnp.where(inner == r, lse_all, 0.0) for r in range(block_rows)], axis=0
    )
    outgoing = lax.dot_general(
        takes,
        stacked,
        (((1,), (1,)), ((), ())),
        preferred_element_type=jnp.float32,
        precision=EXACT,
    )
    lse_out[...] = outgoing.reshape(shards, 1, wide)
    lse_in[pl.ds(me, 1)] = lse_out[pl.ds(me, 1)]

    @pl.loop(1, shards)
    def _(off):
        lse_copy(off).start()

    @pl.loop(1, total)
    def _(off):
        mk_copy(off).wait()

    flag_sum = jnp.sum(mkbuf[...].astype(jnp.float32), axis=0)
    token_total = jnp.sum(flag_sum, axis=1, keepdims=True)
    token_weight[...] = flags[...].astype(jnp.float32) * (float(total * rows) / token_total)

    @pl.loop(1, reach + 1)
    def _(k):
        @pl.when(me + k < shards)
        def _():
            id_copy(k, me + k).wait_send()
            kv_copy(k, me + k).wait_send()

    @pl.loop(1, shards)
    def _(off):
        lse_copy(off).wait()

    arrived = lse_in[...].reshape(shards, wide)
    spread_t = ((iota((rows, shards), 0) >> row_bits) == iota((rows, shards), 1)).astype(
        jnp.float32
    )
    placed = jnp.dot(spread_t, arrived, preferred_element_type=jnp.float32, precision=EXACT)
    keep = (iota((rows, wide), 0) & (block_rows - 1)) == (iota((rows, wide), 1) >> head_bits)
    placed = jnp.where(keep, placed, 0.0)
    pick = ((iota((heads, wide), 1) & (heads - 1)) == iota((heads, wide), 0)).astype(jnp.float32)
    row_lse[0] = lax.dot_general(
        pick, placed, (((1,), (1,)), ((), ())), preferred_element_type=jnp.float32, precision=EXACT
    )


def body(
    parts,
    shards,
    hidden,
    norm_gain,
    query_weight,
    keyval_weight,
    sink_logits,
    document_ids,
    block_owner,
    loss_mask,
):
    rows, model = hidden.shape[1:]
    heads = sink_logits.shape[0]
    kv_width = keyval_weight.shape[1] // 2
    kv_heads = kv_width // HEAD_DIM
    reach = min(-(-(DOC_MOST - 1) // rows), shards - 1)
    total = parts * shards
    wide = (rows // shards) * heads
    width = heads // kv_heads * HEAD_DIM
    tables = [jnp.asarray(t) for t in rope_tables(shards, rows)]
    vmem = pl.BlockSpec(memory_space=pltpu.VMEM)
    hbm = pl.BlockSpec(memory_space=pl.ANY)
    smem = pl.BlockSpec(memory_space=pltpu.SMEM)
    dma = pltpu.SemaphoreType.DMA
    return pl.pallas_call(
        functools.partial(kernel, (parts, shards, reach, heads, kv_heads)),
        out_shape=(
            jax.ShapeDtypeStruct((1, rows, heads * HEAD_DIM), jnp.bfloat16),
            jax.ShapeDtypeStruct((1, heads, rows), jnp.float32),
            jax.ShapeDtypeStruct((1, rows), jnp.float32),
        ),
        in_specs=[vmem, vmem, hbm, hbm, smem, vmem, vmem, vmem] + [vmem] * 4,
        out_specs=(vmem, vmem, vmem),
        scratch_shapes=[
            pltpu.VMEM((kv_heads, model, width), jnp.bfloat16),
            pltpu.VMEM((model, 2 * kv_width), jnp.bfloat16),
            pltpu.VMEM((reach + 1, 2 * kv_width, rows), jnp.bfloat16),
            pltpu.VMEM((reach + 1, 1, rows), jnp.int32),
            pltpu.VMEM((total, 1, rows), jnp.int32),
            pltpu.VMEM((heads // 2, 2 * rows, LANES), jnp.bfloat16),
            pltpu.VMEM(((reach + 1) * rows, rows), jnp.float32),
            pltpu.VMEM((heads, rows), jnp.float32),
            pltpu.VMEM((shards, 1, wide), jnp.float32),
            pltpu.VMEM((shards, 1, wide), jnp.float32),
            dma((kv_heads + 1,)),
            dma((reach,)),
            dma((reach,)),
            dma((reach,)),
            dma((reach,)),
            dma((total - 1,)),
            dma((total - 1,)),
            dma((shards - 1,)),
            dma((shards - 1,)),
        ],
        compiler_params=pltpu.CompilerParams(
            collective_id=0, has_side_effects=True, vmem_limit_bytes=60 * 1024 * 1024
        ),
    )(
        hidden,
        norm_gain.reshape(1, model),
        query_weight,
        keyval_weight,
        sink_logits,
        document_ids,
        block_owner,
        loss_mask,
        *tables,
    )


def solution(mesh):
    in_specs = (
        P("dp", "cp", None),
        P(),
        P(),
        P(),
        P(),
        P("dp", "cp"),
        P("dp", "cp", None),
        P("dp", "cp"),
    )
    out_specs = (P("dp", "cp", None), P("dp", None, "cp"), P("dp", "cp"))
    local = functools.partial(body, mesh.shape["dp"], mesh.shape["cp"])
    return jax.shard_map(local, mesh=mesh, in_specs=in_specs, out_specs=out_specs, check_vma=False)
```

```python
import functools
import math

import jax
import jax.numpy as jnp
import numpy as np
from jax import lax
from jax.experimental import pallas as pl
from jax.experimental.pallas import tpu as pltpu
from jax.sharding import PartitionSpec as P

HEAD_DIM = 64
DOC_MOST = 1024

rope_base = 150000.0
norm_eps = 1e-05
masked_score = -1e30
LANES = 128
LOG2E = math.log2(math.e)
LN2 = math.log(2.0)
MESH = pl.DeviceIdType.MESH
RELAY_AT, HAND_AT = 1, 3
EXACT = lax.Precision.HIGHEST


def iota(shape, axis):
    return lax.broadcasted_iota(jnp.int32, shape, axis)


def rope_tables(shards, own_rows):
    half = HEAD_DIM // 2
    frequency = rope_base ** (-np.arange(half, dtype=np.float64) / half)
    frequency = np.tile(frequency, LANES // half)
    base = np.arange(shards, dtype=np.float64)[:, None] * own_rows * frequency
    row = np.arange(own_rows, dtype=np.float64)[:, None] * frequency
    return [np.asarray(f(x), np.float32) for x in (base, row) for f in (np.cos, np.sin)]


def kernel(
    dims,
    hidden,
    gain,
    wq_hbm,
    wkv_hbm,
    sink,
    ids,
    owner,
    flags,
    cos_base,
    sin_base,
    cos_row,
    sin_row,
    attended,
    row_lse,
    token_weight,
    wq,
    wkv,
    kv,
    idbuf,
    mkbuf,
    queries,
    bias,
    lse,
    lse_out,
    lse_in,
    w_sem,
    kv_send,
    kv_recv,
    id_send,
    id_recv,
    mk_send,
    mk_recv,
    lse_send,
    lse_recv,
):
    parts, shards, reach, heads, kv_heads = dims
    me = lax.axis_index("cp")
    part = lax.axis_index("dp")
    total = parts * shards
    rows = hidden.shape[2]
    group = heads // kv_heads
    width = group * HEAD_DIM
    kv_width = kv_heads * HEAD_DIM
    pairs = heads // 2
    pairs_kv = group // 2
    block_rows = rows // shards
    row_bits = block_rows.bit_length() - 1
    head_bits = heads.bit_length() - 1

    barrier = pltpu.get_barrier_semaphore()

    @pl.loop(1, shards)
    def _(off):
        pl.semaphore_signal(
            barrier, inc=1, device_id={"cp": lax.rem(me + off, shards)}, device_id_type=MESH
        )

    for d in range(1, parts):
        pl.semaphore_signal(
            barrier, inc=1, device_id={"dp": lax.rem(part + d, parts)}, device_id_type=MESH
        )

    kv_load = pltpu.make_async_copy(wkv_hbm, wkv, w_sem.at[kv_heads])
    kv_load.start()
    q_loads = [
        pltpu.make_async_copy(wq_hbm.at[:, pl.ds(c * width, width)], wq.at[c], w_sem.at[c])
        for c in range(kv_heads)
    ]
    for load in q_loads:
        load.start()

    spot = lax.rem(me, reach)
    core = lax.rem(spot, 2)
    chip = spot // 2
    chips = reach // 2
    has_before = me >= reach

    def kv_copy(source, slot, send, target):
        return pltpu.make_async_remote_copy(
            src_ref=kv.at[source],
            dst_ref=kv.at[slot],
            send_sem=kv_send.at[send],
            recv_sem=kv_recv.at[slot],
            device_id={"cp": target},
            device_id_type=MESH,
        )

    def kv_arrive(slot):
        kv_copy(slot, slot, 0, me).wait_recv()

    def along(source):
        return kv_copy(source, 0, 0, me + reach)

    def across(delta, source):
        to_chip = lax.rem(chip - delta + chips, chips)
        return kv_copy(source, 2 * delta, delta, me - spot + 2 * to_chip + core)

    def partner(j, source):
        return kv_copy(source, 2 * j + 1, chips + j, me + 1 - 2 * core)

    def id_copy(k, target):
        return pltpu.make_async_remote_copy(
            src_ref=ids,
            dst_ref=idbuf.at[reach - k],
            send_sem=id_send.at[k - 1],
            recv_sem=id_recv.at[k - 1],
            device_id={"cp": target},
            device_id_type=MESH,
        )

    def mk_copy(d):
        return pltpu.make_async_remote_copy(
            src_ref=flags,
            dst_ref=mkbuf.at[d],
            send_sem=mk_send.at[d - 1],
            recv_sem=mk_recv.at[d - 1],
            device_id={"dp": lax.rem(part + d, parts)},
            device_id_type=MESH,
        )

    def lse_copy(off):
        target = lax.rem(me + off, shards)
        return pltpu.make_async_remote_copy(
            src_ref=lse_out.at[target],
            dst_ref=lse_in.at[me],
            send_sem=lse_send.at[off - 1],
            recv_sem=lse_recv.at[off - 1],
            device_id={"cp": target},
            device_id_type=MESH,
        )

    x = hidden[0].astype(jnp.float32).T
    inv_rms = lax.rsqrt(jnp.mean(x * x, axis=1, keepdims=True) + norm_eps)
    normed = (x * inv_rms * gain[...][None, :]).astype(jnp.bfloat16)

    cb, sb = cos_base[pl.ds(me, 1), :], sin_base[pl.ds(me, 1), :]
    cr, sr = cos_row[...], sin_row[...]
    lane = iota((rows, LANES), 1)
    first_half = (lane & (HEAD_DIM - 1)) < HEAD_DIM // 2
    low = lane < HEAD_DIM
    cosine = cb * cr - sb * sr
    sine = sb * cr + cb * sr
    sine = jnp.where(first_half, -sine, sine)

    def rotate(u):
        swapped = jnp.where(
            first_half,
            pltpu.roll(u, LANES - HEAD_DIM // 2, 1),
            pltpu.roll(u, HEAD_DIM // 2, 1),
        )
        return u * cosine + swapped * sine

    kv_load.wait()
    keyval = jnp.dot(normed, wkv[...], preferred_element_type=jnp.float32)
    for c in range(kv_width // LANES):
        part_k = keyval[:, c * LANES : (c + 1) * LANES]
        kv[reach, c * LANES : (c + 1) * LANES, :] = rotate(part_k).astype(jnp.bfloat16)
        part_v = keyval[:, kv_width + c * LANES : kv_width + (c + 1) * LANES]
        kv[reach, kv_width + c * LANES : kv_width + (c + 1) * LANES, :] = part_v.T.astype(
            jnp.bfloat16
        )
    idbuf[reach] = ids[...]
    mkbuf[0] = flags[...]

    pl.semaphore_wait(barrier, shards + parts - 2)

    @pl.loop(1, reach + 1)
    def _(k):
        @pl.when(me + k < shards)
        def _():
            id_copy(k, me + k).start()

        @pl.when(me - k < 0)
        def _():
            kv[reach - k] = jnp.zeros(kv.shape[1:], kv.dtype)
            idbuf[reach - k] = jnp.full(idbuf.shape[1:], -1, jnp.int32)

    for d in range(1, parts):
        mk_copy(d).start()

    @pl.when(me + reach < shards)
    def _():
        along(reach).start()

    for delta in range(1, chips):

        @pl.when(chip < delta)
        def _():
            across(delta, reach).start()

    @pl.when(core == 0)
    def _():
        partner(chips - 1, reach).start()

    def relay():
        @pl.when(has_before)
        def _():
            kv_arrive(0)
            for delta in range(1, chips):

                @pl.when(chip >= delta)
                def _():
                    across(delta, 0).start()

            @pl.when(core == 1)
            def _():
                partner(0, 0).start()

    def hand_over():
        for delta in reversed(range(1, chips)):

            @pl.when(me + 2 * delta >= reach)
            def _():
                kv_arrive(2 * delta)

                @pl.when(core == 0)
                def _():
                    partner(delta - 1, 2 * delta).start()

                @pl.when(core == 1)
                def _():
                    partner(delta, 2 * delta).start()

    for c in range(kv_heads):
        if c == RELAY_AT:
            relay()
        if c == HAND_AT:
            hand_over()
        q_loads[c].wait()
        projected = jnp.dot(normed, wq[c], preferred_element_type=jnp.float32)
        for j in range(pairs_kv):
            y = rotate(projected[:, j * LANES : (j + 1) * LANES]) * (LOG2E * HEAD_DIM**-0.5)
            yr = pltpu.roll(y, HEAD_DIM, 1)
            if c % 2 == 0:
                one, two = jnp.where(low, y, 0.0), jnp.where(low, yr, 0.0)
            else:
                one, two = jnp.where(low, 0.0, yr), jnp.where(low, 0.0, y)
            queries[c * pairs_kv + j, 0:rows, :] = one.astype(jnp.bfloat16)
            queries[c * pairs_kv + j, rows : 2 * rows, :] = two.astype(jnp.bfloat16)

    @pl.loop(1, reach + 1)
    def _(k):
        @pl.when(me - k >= 0)
        def _():
            id_copy(k, me).wait_recv()

    own_ids = jnp.broadcast_to(ids[...].astype(jnp.float32), (rows, rows))
    for slot in range(reach + 1):
        key_ids = jnp.broadcast_to(idbuf[slot].astype(jnp.float32), (rows, rows)).T
        allowed = key_ids == own_ids
        if slot == reach:
            allowed = allowed & (iota((rows, rows), 0) <= iota((rows, rows), 1))
        bias[slot * rows : (slot + 1) * rows, :] = jnp.where(allowed, 0.0, masked_score)

    for j in range(chips):

        @pl.when(me + 2 * j + 1 >= reach)
        def _():
            kv_arrive(2 * j + 1)

    key_count = (reach + 1) * rows

    def attend(p):
        a = p // pairs_kv
        key_part = kv[:, pl.ds(pl.multiple_of((a // 2) * LANES, LANES), LANES), :]
        key_part = key_part.reshape(key_count, LANES)
        value_rows = pl.ds(pl.multiple_of(kv_width + a * HEAD_DIM, HEAD_DIM), HEAD_DIM)
        values_t = jnp.concatenate([kv[s, value_rows, :] for s in range(reach + 1)], axis=1)
        scores = lax.dot_general(
            key_part, queries[p], (((1,), (1,)), ((), ())), preferred_element_type=jnp.float32
        )
        shift = bias[...]
        scores = scores + jnp.concatenate([shift, shift], axis=1)
        sink_row = jnp.where(
            iota((1, 2 * rows), 1) < rows, sink[2 * p] * LOG2E, sink[2 * p + 1] * LOG2E
        )
        top = jnp.maximum(jnp.max(scores, axis=0, keepdims=True), sink_row)
        weights = jnp.exp2(scores - top)
        row_total = jnp.sum(weights, axis=0, keepdims=True) + jnp.exp2(sink_row - top)
        mixed = jnp.dot(
            values_t, weights.astype(jnp.bfloat16), preferred_element_type=jnp.float32
        )
        mixed = mixed / row_total
        both = jnp.concatenate([mixed[:, :rows], mixed[:, rows:]], axis=0)
        attended[0, :, pl.ds(pl.multiple_of(p * LANES, LANES), LANES)] = both.T.astype(
            jnp.bfloat16
        )
        log_total = top * LN2 + jnp.log(row_total)
        lse[pl.ds(2 * p, 1), :] = log_total[:, :rows]
        lse[pl.ds(2 * p + 1, 1), :] = log_total[:, rows:]

    @pl.loop(0, pairs // 2)
    def _(i):
        attend(2 * i)
        attend(2 * i + 1)

    wide = block_rows * heads
    owner_hot = (jnp.broadcast_to(owner[0], (shards, shards)) == iota((shards, shards), 0)).astype(
        jnp.float32
    )
    spread = ((iota((shards, rows), 1) >> row_bits) == iota((shards, rows), 0)).astype(jnp.float32)
    takes = jnp.dot(owner_hot, spread, preferred_element_type=jnp.float32)
    inner = iota((heads, rows), 1) & (block_rows - 1)
    lse_all = lse[...]
    stacked = jnp.concatenate(
        [jnp.where(inner == r, lse_all, 0.0) for r in range(block_rows)], axis=0
    )
    outgoing = lax.dot_general(
        takes,
        stacked,
        (((1,), (1,)), ((), ())),
        preferred_element_type=jnp.float32,
        precision=EXACT,
    )
    for d in range(1, parts):
        mk_copy(d).wait()
    own_flags = jnp.sum(mkbuf[...].astype(jnp.float32), axis=0)
    lse_out[:, :, 0:wide] = outgoing.reshape(shards, 1, wide)
    lse_out[:, :, wide : wide + rows] = jnp.broadcast_to(own_flags[None], (shards, 1, rows))
    lse_in[pl.ds(me, 1)] = lse_out[pl.ds(me, 1)]

    @pl.loop(1, shards)
    def _(off):
        lse_copy(off).start()

    @pl.loop(1, reach + 1)
    def _(k):
        @pl.when(me + k < shards)
        def _():
            id_copy(k, me + k).wait_send()

    @pl.when(me + reach < shards)
    def _():
        along(reach).wait_send()

    for delta in range(1, chips):

        @pl.when(has_before | (chip < delta))
        def _():
            across(delta, reach).wait_send()

    for j in range(chips):

        @pl.when(me + 2 * j + 2 * (1 - core) >= reach)
        def _():
            partner(j, reach).wait_send()

    @pl.loop(1, shards)
    def _(off):
        lse_copy(off).wait()

    arrived = lse_in[...].reshape(shards, wide + rows)
    flag_sum = jnp.sum(arrived[:, wide:], axis=0, keepdims=True)
    token_total = jnp.sum(flag_sum, axis=1, keepdims=True)
    token_weight[...] = flags[...].astype(jnp.float32) * (float(total * rows) / token_total)
    arrived = arrived[:, :wide]
    spread_t = ((iota((rows, shards), 0) >> row_bits) == iota((rows, shards), 1)).astype(
        jnp.float32
    )
    placed = jnp.dot(spread_t, arrived, preferred_element_type=jnp.float32, precision=EXACT)
    keep = (iota((rows, wide), 0) & (block_rows - 1)) == (iota((rows, wide), 1) >> head_bits)
    placed = jnp.where(keep, placed, 0.0)
    pick = ((iota((heads, wide), 1) & (heads - 1)) == iota((heads, wide), 0)).astype(jnp.float32)
    row_lse[0] = lax.dot_general(
        pick, placed, (((1,), (1,)), ((), ())), preferred_element_type=jnp.float32, precision=EXACT
    )


def body(
    parts,
    shards,
    hidden,
    norm_gain,
    query_weight,
    keyval_weight,
    sink_logits,
    document_ids,
    block_owner,
    loss_mask,
):
    rows, model = hidden.shape[1:]
    heads = sink_logits.shape[0]
    kv_width = keyval_weight.shape[1] // 2
    kv_heads = kv_width // HEAD_DIM
    reach = min(-(-(DOC_MOST - 1) // rows), shards - 1)
    total = parts * shards
    wide = (rows // shards) * heads
    width = heads // kv_heads * HEAD_DIM
    tables = [jnp.asarray(t) for t in rope_tables(shards, rows)]
    vmem = pl.BlockSpec(memory_space=pltpu.VMEM)
    hbm = pl.BlockSpec(memory_space=pl.ANY)
    smem = pl.BlockSpec(memory_space=pltpu.SMEM)
    dma = pltpu.SemaphoreType.DMA
    return pl.pallas_call(
        functools.partial(kernel, (parts, shards, reach, heads, kv_heads)),
        out_shape=(
            jax.ShapeDtypeStruct((1, rows, heads * HEAD_DIM), jnp.bfloat16),
            jax.ShapeDtypeStruct((1, heads, rows), jnp.float32),
            jax.ShapeDtypeStruct((1, rows), jnp.float32),
        ),
        in_specs=[vmem, vmem, hbm, hbm, smem, vmem, vmem, vmem] + [vmem] * 4,
        out_specs=(vmem, vmem, vmem),
        scratch_shapes=[
            pltpu.VMEM((kv_heads, model, width), jnp.bfloat16),
            pltpu.VMEM((model, 2 * kv_width), jnp.bfloat16),
            pltpu.VMEM((reach + 1, 2 * kv_width, rows), jnp.bfloat16),
            pltpu.VMEM((reach + 1, 1, rows), jnp.int32),
            pltpu.VMEM((parts, 1, rows), jnp.int32),
            pltpu.VMEM((heads // 2, 2 * rows, LANES), jnp.bfloat16),
            pltpu.VMEM(((reach + 1) * rows, rows), jnp.float32),
            pltpu.VMEM((heads, rows), jnp.float32),
            pltpu.VMEM((shards, 1, wide + rows), jnp.float32),
            pltpu.VMEM((shards, 1, wide + rows), jnp.float32),
            dma((kv_heads + 1,)),
            dma((reach,)),
            dma((reach,)),
            dma((reach,)),
            dma((reach,)),
            dma((max(parts - 1, 1),)),
            dma((max(parts - 1, 1),)),
            dma((shards - 1,)),
            dma((shards - 1,)),
        ],
        compiler_params=pltpu.CompilerParams(
            collective_id=0, has_side_effects=True, vmem_limit_bytes=60 * 1024 * 1024
        ),
    )(
        jnp.swapaxes(hidden, 1, 2),
        norm_gain,
        query_weight,
        keyval_weight,
        sink_logits,
        document_ids,
        block_owner,
        loss_mask,
        *tables,
    )


def solution(mesh):
    in_specs = (
        P("dp", "cp", None),
        P(),
        P(),
        P(),
        P(),
        P("dp", "cp"),
        P("dp", "cp", None),
        P("dp", "cp"),
    )
    out_specs = (P("dp", "cp", None), P("dp", None, "cp"), P("dp", "cp"))
    local = functools.partial(body, mesh.shape["dp"], mesh.shape["cp"])
    return jax.shard_map(local, mesh=mesh, in_specs=in_specs, out_specs=out_specs, check_vma=False)
```

```python
import functools
import math

import jax
import jax.numpy as jnp
import numpy as np
from jax import lax
from jax.experimental import pallas as pl
from jax.experimental.pallas import tpu as pltpu
from jax.sharding import PartitionSpec as P

HEAD_DIM = 64
DOC_MOST = 1024

rope_base = 150000.0
norm_eps = 1e-05
masked_score = -1e30
LANES = 128
LOG2E = math.log2(math.e)
LN2 = math.log(2.0)
MESH = pl.DeviceIdType.MESH
RELAY_AT, HAND_AT = 1, 3
EXACT = lax.Precision.HIGHEST


def iota(shape, axis):
    return lax.broadcasted_iota(jnp.int32, shape, axis)


def rope_tables(shards, own_rows):
    half = HEAD_DIM // 2
    frequency = rope_base ** (-np.arange(half, dtype=np.float64) / half)
    frequency = np.tile(frequency, LANES // half)
    base = np.arange(shards, dtype=np.float64)[:, None] * own_rows * frequency
    row = np.arange(own_rows, dtype=np.float64)[:, None] * frequency
    return [np.asarray(f(x), np.float32) for x in (base, row) for f in (np.cos, np.sin)]


def kernel(
    dims,
    hidden,
    gain,
    wq_hbm,
    wkv_hbm,
    sink,
    ids,
    owner,
    flags,
    cos_base,
    sin_base,
    cos_row,
    sin_row,
    attended,
    row_lse,
    token_weight,
    wq,
    wkv,
    kv,
    idbuf,
    mkbuf,
    queries,
    bias,
    lse,
    lse_out,
    lse_in,
    w_sem,
    kv_send,
    kv_recv,
    id_send,
    id_recv,
    mk_send,
    mk_recv,
    lse_send,
    lse_recv,
    hid,
):
    parts, shards, reach, heads, kv_heads = dims
    me = lax.axis_index("cp")
    part = lax.axis_index("dp")
    total = parts * shards
    rows = hidden.shape[2]
    group = heads // kv_heads
    width = group * HEAD_DIM
    kv_width = kv_heads * HEAD_DIM
    pairs = heads // 2
    pairs_kv = group // 2
    block_rows = rows // shards
    row_bits = block_rows.bit_length() - 1
    head_bits = heads.bit_length() - 1

    barrier = pltpu.get_barrier_semaphore()

    @pl.loop(1, shards)
    def _(off):
        pl.semaphore_signal(
            barrier, inc=1, device_id={"cp": lax.rem(me + off, shards)}, device_id_type=MESH
        )

    for d in range(1, parts):
        pl.semaphore_signal(
            barrier, inc=1, device_id={"dp": lax.rem(part + d, parts)}, device_id_type=MESH
        )

    kv_load = pltpu.make_async_copy(wkv_hbm, wkv, w_sem.at[kv_heads])
    hid_load = pltpu.make_async_copy(hidden.at[0], hid, w_sem.at[kv_heads + 1])
    hid_load.start()
    kv_load.start()
    q_loads = [
        pltpu.make_async_copy(wq_hbm.at[:, pl.ds(c * width, width)], wq.at[c], w_sem.at[c])
        for c in range(kv_heads)
    ]

    spot = lax.rem(me, reach)
    core = lax.rem(spot, 2)
    chip = spot // 2
    chips = reach // 2
    has_before = me >= reach

    def kv_copy(source, slot, send, target):
        return pltpu.make_async_remote_copy(
            src_ref=kv.at[source],
            dst_ref=kv.at[slot],
            send_sem=kv_send.at[send],
            recv_sem=kv_recv.at[slot],
            device_id={"cp": target},
            device_id_type=MESH,
        )

    def kv_arrive(slot):
        kv_copy(slot, slot, 0, me).wait_recv()

    def along(source):
        return kv_copy(source, 0, 0, me + reach)

    def across(delta, source):
        to_chip = lax.rem(chip - delta + chips, chips)
        return kv_copy(source, 2 * delta, delta, me - spot + 2 * to_chip + core)

    def partner(j, source):
        return kv_copy(source, 2 * j + 1, chips + j, me + 1 - 2 * core)

    def id_copy(k, target):
        return pltpu.make_async_remote_copy(
            src_ref=ids,
            dst_ref=idbuf.at[reach - k],
            send_sem=id_send.at[k - 1],
            recv_sem=id_recv.at[k - 1],
            device_id={"cp": target},
            device_id_type=MESH,
        )

    def mk_copy(d):
        return pltpu.make_async_remote_copy(
            src_ref=flags,
            dst_ref=mkbuf.at[d],
            send_sem=mk_send.at[d - 1],
            recv_sem=mk_recv.at[d - 1],
            device_id={"dp": lax.rem(part + d, parts)},
            device_id_type=MESH,
        )

    def lse_copy(off):
        target = lax.rem(me + off, shards)
        return pltpu.make_async_remote_copy(
            src_ref=lse_out.at[target],
            dst_ref=lse_in.at[me],
            send_sem=lse_send.at[off - 1],
            recv_sem=lse_recv.at[off - 1],
            device_id={"cp": target},
            device_id_type=MESH,
        )

    hid_load.wait()
    x = hid[...].astype(jnp.float32).T
    inv_rms = lax.rsqrt(jnp.mean(x * x, axis=1, keepdims=True) + norm_eps)
    normed = (x * inv_rms * gain[...][None, :]).astype(jnp.bfloat16)

    cb, sb = cos_base[pl.ds(me, 1), :], sin_base[pl.ds(me, 1), :]
    cr, sr = cos_row[...], sin_row[...]
    lane = iota((rows, LANES), 1)
    first_half = (lane & (HEAD_DIM - 1)) < HEAD_DIM // 2
    low = lane < HEAD_DIM
    cosine = cb * cr - sb * sr
    sine = sb * cr + cb * sr
    sine = jnp.where(first_half, -sine, sine)

    def rotate(u):
        swapped = jnp.where(
            first_half,
            pltpu.roll(u, LANES - HEAD_DIM // 2, 1),
            pltpu.roll(u, HEAD_DIM // 2, 1),
        )
        return u * cosine + swapped * sine

    kv_load.wait()
    for load in q_loads:
        load.start()
    keyval = jnp.dot(normed, wkv[...], preferred_element_type=jnp.float32)
    for c in range(kv_width // LANES):
        part_k = keyval[:, c * LANES : (c + 1) * LANES]
        kv[reach, c * LANES : (c + 1) * LANES, :] = rotate(part_k).astype(jnp.bfloat16)
        part_v = keyval[:, kv_width + c * LANES : kv_width + (c + 1) * LANES]
        kv[reach, kv_width + c * LANES : kv_width + (c + 1) * LANES, :] = part_v.T.astype(
            jnp.bfloat16
        )
    idbuf[reach] = ids[...]
    mkbuf[0] = flags[...]

    pl.semaphore_wait(barrier, shards + parts - 2)

    @pl.loop(1, reach + 1)
    def _(k):
        @pl.when(me + k < shards)
        def _():
            id_copy(k, me + k).start()

        @pl.when(me - k < 0)
        def _():
            kv[reach - k] = jnp.zeros(kv.shape[1:], kv.dtype)
            idbuf[reach - k] = jnp.full(idbuf.shape[1:], -1, jnp.int32)

    for d in range(1, parts):
        mk_copy(d).start()

    @pl.when(me + reach < shards)
    def _():
        along(reach).start()

    for delta in range(1, chips):

        @pl.when(chip < delta)
        def _():
            across(delta, reach).start()

    @pl.when(core == 0)
    def _():
        partner(chips - 1, reach).start()

    def relay():
        @pl.when(has_before)
        def _():
            kv_arrive(0)
            for delta in range(1, chips):

                @pl.when(chip >= delta)
                def _():
                    across(delta, 0).start()

            @pl.when(core == 1)
            def _():
                partner(0, 0).start()

    def hand_over():
        for delta in reversed(range(1, chips)):

            @pl.when(me + 2 * delta >= reach)
            def _():
                kv_arrive(2 * delta)

                @pl.when(core == 0)
                def _():
                    partner(delta - 1, 2 * delta).start()

                @pl.when(core == 1)
                def _():
                    partner(delta, 2 * delta).start()

    for c in range(kv_heads):
        if c == RELAY_AT:
            relay()
        if c == HAND_AT:
            hand_over()
        q_loads[c].wait()
        projected = jnp.dot(normed, wq[c], preferred_element_type=jnp.float32)
        for j in range(pairs_kv):
            y = rotate(projected[:, j * LANES : (j + 1) * LANES]) * (LOG2E * HEAD_DIM**-0.5)
            yr = pltpu.roll(y, HEAD_DIM, 1)
            if c % 2 == 0:
                one, two = jnp.where(low, y, 0.0), jnp.where(low, yr, 0.0)
            else:
                one, two = jnp.where(low, 0.0, yr), jnp.where(low, 0.0, y)
            queries[c * pairs_kv + j, 0:rows, :] = one.astype(jnp.bfloat16)
            queries[c * pairs_kv + j, rows : 2 * rows, :] = two.astype(jnp.bfloat16)

    @pl.loop(1, reach + 1)
    def _(k):
        @pl.when(me - k >= 0)
        def _():
            id_copy(k, me).wait_recv()

    own_ids = jnp.broadcast_to(ids[...].astype(jnp.float32), (rows, rows))
    for slot in range(reach + 1):
        key_ids = jnp.broadcast_to(idbuf[slot].astype(jnp.float32), (rows, rows)).T
        allowed = key_ids == own_ids
        if slot == reach:
            allowed = allowed & (iota((rows, rows), 0) <= iota((rows, rows), 1))
        bias[slot * rows : (slot + 1) * rows, :] = jnp.where(allowed, 0.0, masked_score)

    for j in range(chips):

        @pl.when(me + 2 * j + 1 >= reach)
        def _():
            kv_arrive(2 * j + 1)

    key_count = (reach + 1) * rows

    def attend(p):
        a = p // pairs_kv
        key_part = kv[:, pl.ds(pl.multiple_of((a // 2) * LANES, LANES), LANES), :]
        key_part = key_part.reshape(key_count, LANES)
        value_rows = pl.ds(pl.multiple_of(kv_width + a * HEAD_DIM, HEAD_DIM), HEAD_DIM)
        values_t = jnp.concatenate([kv[s, value_rows, :] for s in range(reach + 1)], axis=1)
        scores = lax.dot_general(
            key_part, queries[p], (((1,), (1,)), ((), ())), preferred_element_type=jnp.float32
        )
        shift = bias[...]
        scores = scores + jnp.concatenate([shift, shift], axis=1)
        sink_row = jnp.where(
            iota((1, 2 * rows), 1) < rows, sink[2 * p] * LOG2E, sink[2 * p + 1] * LOG2E
        )
        top = jnp.maximum(jnp.max(scores, axis=0, keepdims=True), sink_row)
        weights = jnp.exp2(scores - top)
        row_total = jnp.sum(weights, axis=0, keepdims=True) + jnp.exp2(sink_row - top)
        mixed = jnp.dot(
            values_t, weights.astype(jnp.bfloat16), preferred_element_type=jnp.float32
        )
        mixed = mixed * (1.0 / row_total)
        both = jnp.concatenate([mixed[:, :rows], mixed[:, rows:]], axis=0)
        attended[0, :, pl.ds(pl.multiple_of(p * LANES, LANES), LANES)] = both.T.astype(
            jnp.bfloat16
        )
        log_total = top * LN2 + jnp.log(row_total)
        lse[pl.ds(2 * p, 1), :] = log_total[:, :rows]
        lse[pl.ds(2 * p + 1, 1), :] = log_total[:, rows:]

    @pl.loop(0, pairs // pairs_kv)
    def _(i):
        for j in range(pairs_kv):
            attend(pairs_kv * i + j)

    wide = block_rows * heads
    owner_hot = (jnp.broadcast_to(owner[0], (shards, shards)) == iota((shards, shards), 0)).astype(
        jnp.float32
    )
    spread = ((iota((shards, rows), 1) >> row_bits) == iota((shards, rows), 0)).astype(jnp.float32)
    takes = jnp.dot(owner_hot, spread, preferred_element_type=jnp.float32)
    inner = iota((heads, rows), 1) & (block_rows - 1)
    lse_all = lse[...]
    stacked = jnp.concatenate(
        [jnp.where(inner == r, lse_all, 0.0) for r in range(block_rows)], axis=0
    )
    outgoing = lax.dot_general(
        takes,
        stacked,
        (((1,), (1,)), ((), ())),
        preferred_element_type=jnp.float32,
        precision=EXACT,
    )
    for d in range(1, parts):
        mk_copy(d).wait()
    own_flags = jnp.sum(mkbuf[...].astype(jnp.float32), axis=0)
    lse_out[:, :, 0:wide] = outgoing.reshape(shards, 1, wide)
    lse_out[:, :, wide : wide + rows] = jnp.broadcast_to(own_flags[None], (shards, 1, rows))
    lse_in[pl.ds(me, 1)] = lse_out[pl.ds(me, 1)]

    @pl.loop(1, shards)
    def _(off):
        lse_copy(off).start()

    @pl.loop(1, reach + 1)
    def _(k):
        @pl.when(me + k < shards)
        def _():
            id_copy(k, me + k).wait_send()

    @pl.when(me + reach < shards)
    def _():
        along(reach).wait_send()

    for delta in range(1, chips):

        @pl.when(has_before | (chip < delta))
        def _():
            across(delta, reach).wait_send()

    for j in range(chips):

        @pl.when(me + 2 * j + 2 * (1 - core) >= reach)
        def _():
            partner(j, reach).wait_send()

    @pl.loop(1, shards)
    def _(off):
        lse_copy(off).wait()

    arrived = lse_in[...].reshape(shards, wide + rows)
    flag_sum = jnp.sum(arrived[:, wide:], axis=0, keepdims=True)
    token_total = jnp.sum(flag_sum, axis=1, keepdims=True)
    token_weight[...] = flags[...].astype(jnp.float32) * (float(total * rows) / token_total)
    arrived = arrived[:, :wide]
    spread_t = ((iota((rows, shards), 0) >> row_bits) == iota((rows, shards), 1)).astype(
        jnp.float32
    )
    placed = jnp.dot(spread_t, arrived, preferred_element_type=jnp.float32, precision=EXACT)
    keep = (iota((rows, wide), 0) & (block_rows - 1)) == (iota((rows, wide), 1) >> head_bits)
    placed = jnp.where(keep, placed, 0.0)
    pick = ((iota((heads, wide), 1) & (heads - 1)) == iota((heads, wide), 0)).astype(jnp.float32)
    row_lse[0] = lax.dot_general(
        pick, placed, (((1,), (1,)), ((), ())), preferred_element_type=jnp.float32, precision=EXACT
    )


def body(
    parts,
    shards,
    hidden,
    norm_gain,
    query_weight,
    keyval_weight,
    sink_logits,
    document_ids,
    block_owner,
    loss_mask,
):
    rows, model = hidden.shape[1:]
    heads = sink_logits.shape[0]
    kv_width = keyval_weight.shape[1] // 2
    kv_heads = kv_width // HEAD_DIM
    reach = min(-(-(DOC_MOST - 1) // rows), shards - 1)
    total = parts * shards
    wide = (rows // shards) * heads
    width = heads // kv_heads * HEAD_DIM
    tables = [jnp.asarray(t) for t in rope_tables(shards, rows)]
    vmem = pl.BlockSpec(memory_space=pltpu.VMEM)
    hbm = pl.BlockSpec(memory_space=pl.ANY)
    smem = pl.BlockSpec(memory_space=pltpu.SMEM)
    dma = pltpu.SemaphoreType.DMA
    return pl.pallas_call(
        functools.partial(kernel, (parts, shards, reach, heads, kv_heads)),
        out_shape=(
            jax.ShapeDtypeStruct((1, rows, heads * HEAD_DIM), jnp.bfloat16),
            jax.ShapeDtypeStruct((1, heads, rows), jnp.float32),
            jax.ShapeDtypeStruct((1, rows), jnp.float32),
        ),
        in_specs=[hbm, vmem, hbm, hbm, smem, vmem, vmem, vmem] + [vmem] * 4,
        out_specs=(vmem, vmem, vmem),
        scratch_shapes=[
            pltpu.VMEM((kv_heads, model, width), jnp.bfloat16),
            pltpu.VMEM((model, 2 * kv_width), jnp.bfloat16),
            pltpu.VMEM((reach + 1, 2 * kv_width, rows), jnp.bfloat16),
            pltpu.VMEM((reach + 1, 1, rows), jnp.int32),
            pltpu.VMEM((parts, 1, rows), jnp.int32),
            pltpu.VMEM((heads // 2, 2 * rows, LANES), jnp.bfloat16),
            pltpu.VMEM(((reach + 1) * rows, rows), jnp.float32),
            pltpu.VMEM((heads, rows), jnp.float32),
            pltpu.VMEM((shards, 1, wide + rows), jnp.float32),
            pltpu.VMEM((shards, 1, wide + rows), jnp.float32),
            dma((kv_heads + 2,)),
            dma((reach,)),
            dma((reach,)),
            dma((reach,)),
            dma((reach,)),
            dma((max(parts - 1, 1),)),
            dma((max(parts - 1, 1),)),
            dma((shards - 1,)),
            dma((shards - 1,)),
            pltpu.VMEM((model, rows), jnp.bfloat16),
        ],
        compiler_params=pltpu.CompilerParams(
            collective_id=0, has_side_effects=True, vmem_limit_bytes=60 * 1024 * 1024
        ),
    )(
        jnp.swapaxes(hidden, 1, 2),
        norm_gain,
        query_weight,
        keyval_weight,
        sink_logits,
        document_ids,
        block_owner,
        loss_mask,
        *tables,
    )


def solution(mesh):
    in_specs = (
        P("dp", "cp", None),
        P(),
        P(),
        P(),
        P(),
        P("dp", "cp"),
        P("dp", "cp", None),
        P("dp", "cp"),
    )
    out_specs = (P("dp", "cp", None), P("dp", None, "cp"), P("dp", "cp"))
    local = functools.partial(body, mesh.shape["dp"], mesh.shape["cp"])
    return jax.shard_map(local, mesh=mesh, in_specs=in_specs, out_specs=out_specs, check_vma=False)
```
